128 devices in a mesh: member: 1, lon: 2 (over core), lat: 64 (over z, y, x).
Axes of the slice: x: 4, y: 4, z: 4, core: 2. Of those that a mesh axis runs over, the one named last changes fastest.
Arguments:
- field_in: float32 [1, 128, 384, 768], P('member', None, 'lat', 'lon')
- fwd_table: float32 [256, 256, 384], replicated
- inv_table: float32 [256, 256, 384], replicated
- mix_weights: float32 [256, 128, 128, 2], replicated
Outputs:
- output: float32 [1, 128, 384, 768], P('member', None, 'lat', 'lon')
All inputs are finite; a program needn't handle non-finite values.
Results may differ from the reference program's by a relative error of at most 0.00425.
Values are sent between devices in bfloat16 or wider.
A program may use at most 1 GiB of HBM per device.

```python
import math
import jax
import jax.numpy as jnp
from jax import lax

SAMPLES = 1
CHANNELS = 128
LATITUDES = 384
DEGREES = 256
LONGITUDES = 2 * LATITUDES


def as_bf16(values):
    return values.astype(jnp.bfloat16).astype(jnp.float32)


def legendre_table(colatitude):
    cos_t = jnp.cos(colatitude)
    log_sin = jnp.log(jnp.sin(colatitude))
    orders = jnp.arange(DEGREES).astype(jnp.float32)
    log_steps = jnp.cumsum(jnp.log((2.0 * orders + 1.0) / (2.0 * orders + 2.0)))
    log_prod = jnp.concatenate([jnp.zeros((1,), jnp.float32), log_steps[:-1]])
    log_diag = 0.5 * (jnp.log((2.0 * orders + 1.0) / (4.0 * math.pi)) + log_prod)
    diag_vals = jnp.exp(log_diag[:, None] + orders[:, None] * log_sin[None, :])

    def degree_step(carry_vals, degree):
        prev_two, prev_one = carry_vals
        deg_f = degree.astype(jnp.float32)
        coef_a = jnp.sqrt(jnp.maximum(4.0 * deg_f * deg_f - 1.0, 0.0) / jnp.maximum(deg_f * deg_f - orders * orders, 1.0))
        prev_f = deg_f - 1.0
        coef_b = jnp.sqrt(jnp.maximum(prev_f * prev_f - orders * orders, 0.0) / jnp.maximum(4.0 * prev_f * prev_f - 1.0, 1.0))
        recur_val = coef_a[:, None] * (cos_t[None, :] * prev_one - coef_b[:, None] * prev_two)
        next_val = jnp.where((deg_f == orders)[:, None], diag_vals, jnp.where((deg_f > orders)[:, None], recur_val, 0.0))
        return (prev_one, next_val), next_val

    zero_rows = jnp.zeros((DEGREES, LATITUDES), jnp.float32)
    _, leg_table = lax.scan(degree_step, (zero_rows, zero_rows), jnp.arange(DEGREES))
    return jnp.transpose(leg_table, (1, 0, 2))


def setup_inputs(seed: int = 0, part: int = 0) -> dict:
    root_key = jax.random.key(seed)
    key_field, key_fwd, key_inv, key_mix = jax.random.split(root_key, 4)
    key_part = jax.random.fold_in(key_field, part)
    key_noise, key_smooth = jax.random.split(key_part, 2)
    colatitude = math.pi * (jnp.arange(LATITUDES).astype(jnp.float32) + 0.5) / LATITUDES
    longitude = (2.0 * math.pi / LONGITUDES) * jnp.arange(LONGITUDES).astype(jnp.float32)
    smooth_coef = jax.random.normal(key_smooth, (SAMPLES, CHANNELS, 3, 1, 1), jnp.float32)
    smooth = smooth_coef[:, :, 0] * jnp.cos(colatitude)[:, None] + jnp.sin(colatitude)[:, None] * (smooth_coef[:, :, 1] * jnp.cos(longitude) + smooth_coef[:, :, 2] * jnp.sin(longitude))
    white_noise = jax.random.normal(key_noise, (SAMPLES, CHANNELS, LATITUDES, LONGITUDES), jnp.float32)
    field_in = smooth + white_noise
    leg_table = legendre_table(colatitude)
    quad_weights = (2.0 * math.pi / LONGITUDES) * (math.pi / LATITUDES) * jnp.sin(colatitude)
    table_shape = (DEGREES, DEGREES, LATITUDES)
    fwd_table = leg_table * quad_weights * (1.0 + 0.3 * jax.random.uniform(key_fwd, table_shape, jnp.float32, -1.0, 1.0))
    inv_table = leg_table * (1.0 + 0.3 * jax.random.uniform(key_inv, table_shape, jnp.float32, -1.0, 1.0))
    mix_scale = LATITUDES / (DEGREES * math.sqrt(CHANNELS))
    mix_weights = mix_scale * jax.random.normal(key_mix, (DEGREES, CHANNELS, CHANNELS, 2), jnp.float32)
    return {'field_in': field_in, 'fwd_table': fwd_table, 'inv_table': inv_table, 'mix_weights': mix_weights}


def reference(field_in, fwd_table, inv_table, mix_weights):
    lon_ids = jnp.arange(LONGITUDES)
    wave_ids = jnp.arange(DEGREES)
    phase_arg = (2.0 * math.pi / LONGITUDES) * ((lon_ids[:, None] * wave_ids[None, :]) % LONGITUDES).astype(jnp.float32)
    weight_m = jnp.where(wave_ids == 0, 1.0, 2.0).astype(jnp.float32)
    cos_fwd = as_bf16(jnp.cos(phase_arg))
    sin_fwd = as_bf16(-jnp.sin(phase_arg))
    cos_inv = as_bf16(weight_m * jnp.cos(phase_arg))
    sin_inv = as_bf16(-weight_m * jnp.sin(phase_arg))
    fwd_bf = as_bf16(fwd_table)
    inv_bf = as_bf16(inv_table)
    w_re = as_bf16(mix_weights[..., 0])
    w_im = as_bf16(mix_weights[..., 1])

    def one_sample(sample):
        grid_val = as_bf16(sample)
        spec_re = as_bf16(jnp.einsum('ctj,jm->ctm', grid_val, cos_fwd))
        spec_im = as_bf16(jnp.einsum('ctj,jm->ctm', grid_val, sin_fwd))
        coef_re = as_bf16(jnp.einsum('mlt,ctm->clm', fwd_bf, spec_re))
        coef_im = as_bf16(jnp.einsum('mlt,ctm->clm', fwd_bf, spec_im))
        mixed_re = as_bf16(jnp.einsum('loi,ilm->olm', w_re, coef_re) - jnp.einsum('loi,ilm->olm', w_im, coef_im))
        mixed_im = as_bf16(jnp.einsum('loi,ilm->olm', w_re, coef_im) + jnp.einsum('loi,ilm->olm', w_im, coef_re))
        back_re = as_bf16(jnp.einsum('mlt,clm->ctm', inv_bf, mixed_re))
        back_im = as_bf16(jnp.einsum('mlt,clm->ctm', inv_bf, mixed_im))
        wave_grid = as_bf16(jnp.einsum('ctm,jm->ctj', back_re, cos_inv) + jnp.einsum('ctm,jm->ctj', back_im, sin_inv))
        return sample + jax.nn.gelu(wave_grid, approximate=True)

    return lax.map(one_sample, field_in)
```

```python
import functools
import math
import jax
import jax.numpy as jnp
import numpy as np
from jax import lax
from jax.experimental import pallas as pl
from jax.experimental.pallas import tpu as pltpu
from jax.sharding import PartitionSpec as P

MESH = pl.DeviceIdType.MESH
BF = jnp.bfloat16
F32 = jnp.float32
CH = 128
DEV = 128
CHIPS = 64
TT = 3
JH = 384
DEG = 256
LAT = 384
WCH = 8
WSLOTS = 16
EARLY = 3
BLOCKS = DEG // WCH
GROUP = 64


def chip_order():
    hops = lambda o: sum(min(v, 4 - v) for v in o)
    offsets = [(a, b, c) for a in range(4) for b in range(4) for c in range(4) if a or b or c]
    return sorted(offsets, key=lambda o: (-hops(o), o[2], o[0], o[1]))


ORDER = chip_order()


def pair_of_device():
    q = np.arange(CHIPS)
    colour = (q // 16 + q // 4 % 4 + q % 4) % 2
    chip_pair = colour * (CHIPS // 2) + q // 2
    return (2 * chip_pair[:, None] + np.arange(2)[None, :]).reshape(DEV)


def dft_tables():
    lon_points, waves = 2 * JH, DEG
    phase = np.float32(2.0 * math.pi / lon_points) * (
        (np.arange(waves)[:, None] * np.arange(lon_points)[None, :]) % lon_points).astype(np.float32)
    cos_val, sin_val = np.cos(phase), np.sin(phase)
    k = np.where(np.arange(waves) == 0, 1.0, 2.0).astype(np.float32)[:, None]
    fwd = np.stack([cos_val, -sin_val], axis=1).reshape(2 * waves, lon_points)
    inv = np.stack([k * cos_val, -k * sin_val], axis=1).reshape(2 * waves, lon_points)
    rows = (4 * pair_of_device()[:, None] + np.arange(4)[None, :]).reshape(2 * waves)
    return fwd[rows].astype(BF), inv[rows].astype(BF)


def dot(a, b, ca, cb):
    return lax.dot_general(a, b, (((ca,), (cb,)), ((), ())), preferred_element_type=F32)


def kernel(x_hbm, fwd_hbm, inv_hbm, mix_hbm, dftf_hbm, dfti_hbm, y_ref,
           xv, xb, xr, dftf, dfti, acc, sbuf, rbuf, tabf, tabi, tf, ti, wbuf, wt, gat, xm,
           zf, bf, bfull, sbuf2, rbuf2, rbt, ysend, lsem, wsem, xsem, a1sem, a2sem, yesem):
    h = lax.axis_index("lon")
    p = lax.axis_index("lat")
    d = p * 2 + h
    mate = (0, 1 - h, p)

    def wrap(v):
        return jnp.where(v >= 4, v - 4, v)
    z, y, x = lax.div(p, 16), lax.rem(lax.div(p, 4), 4), lax.rem(p, 4)
    zq = [wrap(z + i) * 16 for i in range(4)]
    yq = [wrap(y + i) * 4 for i in range(4)]
    xq = [wrap(x + i) for i in range(4)]

    pair = 2 * (lax.rem(z + y + x, 2) * (CHIPS // 2) + lax.div(p, 2)) + h

    loads = [
        pltpu.make_async_copy(x_hbm, xv, lsem.at[0]),
        pltpu.make_async_copy(dftf_hbm, dftf, lsem.at[1]),
        pltpu.make_async_copy(fwd_hbm.at[pl.ds(2 * pair, 2)], tabf, lsem.at[2]),
        pltpu.make_async_copy(inv_hbm.at[pl.ds(2 * pair, 2)], tabi, lsem.at[3]),
        pltpu.make_async_copy(dfti_hbm, dfti, lsem.at[4]),
    ]
    loads[0].start()

    barrier = pltpu.get_barrier_semaphore()
    for a, b, c in ORDER:
        for e in range(2):
            pl.semaphore_signal(barrier, inc=1, device_id=(0, e, zq[a] + yq[b] + xq[c]), device_id_type=MESH)
    pl.semaphore_signal(barrier, inc=1, device_id=mate, device_id_type=MESH)
    for c in loads[1:]:
        c.start()

    def wcopy(i, slot):
        return pltpu.make_async_copy(mix_hbm.at[pl.ds(i * WCH, WCH)], wbuf.at[slot], wsem.at[slot])

    loads[0].wait()
    for u in range(2):
        for t in range(TT):
            xb[u, pl.ds(t * CH, CH), :] = xv[u * TT + t].astype(BF)
    for i in range(WSLOTS):
        wcopy(i, i).start()
    loads[1].wait()
    own = pl.ds(pl.multiple_of(h * JH, JH), JH)
    oth = pl.ds(pl.multiple_of((1 - h) * JH, JH), JH)
    acc[...] = dot(dftf[:, own], xb[h], 1, 1)

    krow = lax.broadcasted_iota(jnp.int32, (LAT, LAT), 0)
    tcol = lax.broadcasted_iota(jnp.int32, (LAT, LAT), 1)
    perm = jnp.where(tcol == TT * (krow % DEV) + krow // DEV, 1.0, 0.0).astype(BF)
    loads[2].wait()
    loads[3].wait()
    for m in range(2):
        tf[m] = dot(tabf[m].astype(BF), perm, 1, 1).astype(BF)
        ti[m] = dot(perm, tabi[m].astype(BF), 1, 1).astype(BF)

    def prepare(i, refill):
        slot = lax.rem(i, WSLOTS)
        wcopy(i, slot).wait()

        def prep(l, _):
            for q in range(2):
                w = wbuf[slot, l, pl.ds(q, CH, stride=2), :]
                wt[i * WCH + l, :, q * CH:(q + 1) * CH] = w.astype(BF).T
            return 0
        lax.fori_loop(0, WCH, prep, 0, unroll=True)
        if refill:
            wcopy(i + WSLOTS, slot).start()

    def prepare_blocks(lo, hi, refill):
        def one(i, _):
            prepare(i, refill)
            return 0
        lax.fori_loop(lo, hi, one, 0)

    prepare_blocks(0, EARLY, True)
    bf[...] = jnp.zeros_like(bf)
    pl.semaphore_wait(barrier, DEV - 1)
    xcopy = [pltpu.make_async_remote_copy(xb.at[1 - h, pl.ds(t * CH, CH)], xr.at[pl.ds(t * CH, CH)], xsem.at[t], xsem.at[TT + t],
                                          device_id=mate, device_id_type=MESH) for t in range(TT)]
    for c in xcopy:
        c.start()
    for t in range(TT):
        xcopy[t].wait_recv()
    sbuf[...] = (acc[...] + dot(dftf[:, oth], xr[...], 1, 1)).astype(BF).reshape(DEV, 4, TT * CH)

    def exchange(src, dst, sem):
        for a, b, c in ORDER:
            q = zq[a] + yq[b] + xq[c]
            for e in range(2):
                pltpu.make_async_remote_copy(src.at[2 * q + e], dst.at[d], sem.at[0], sem.at[1],
                                             device_id=(0, e, q), device_id_type=MESH).start()
        pltpu.make_async_remote_copy(src.at[d + 1 - 2 * h], dst.at[d], sem.at[0], sem.at[1],
                                     device_id=mate, device_id_type=MESH).start()
        dst[d] = src[d]
        return pltpu.make_async_remote_copy(src.at[pl.ds(0, DEV - 1)], dst.at[pl.ds(0, DEV - 1)], sem.at[0], sem.at[1],
                                            device_id=mate, device_id_type=MESH)

    first = exchange(sbuf, rbuf, a1sem)

    prepare_blocks(EARLY, BLOCKS - WSLOTS, True)
    prepare_blocks(BLOCKS - WSLOTS, BLOCKS, False)

    first.wait_recv()

    for t in range(TT):
        gat[t] = rbuf[:, :, t * CH:(t + 1) * CH].astype(F32).reshape(4 * DEV, CH)
    for m in range(2):
        for r in range(2):
            for t in range(TT):
                xm[m, t * DEV:(t + 1) * DEV, r * CH:(r + 1) * CH] = gat[t, pl.ds(2 * m + r, DEV, stride=4), :].astype(BF)
    for m in range(2):
        coef = dot(tf[m], xm[m], 1, 0)
        for r in range(2):
            zf[pl.ds(2 * r + m, DEG, stride=4), :] = coef[:, r * CH:(r + 1) * CH]

    row = lax.broadcasted_iota(jnp.int32, (8, CH), 0)
    real = lax.rem(row, 4) < 2
    sign = jnp.where(real, -1.0, 1.0)
    low = lax.broadcasted_iota(jnp.int32, (8, 2 * CH), 0) < 4

    def mix(group, _):
        for u in range(GROUP):
            l = group * GROUP + u
            rows = pl.ds(pl.multiple_of(8 * l, 8), 8)
            coef = zf[rows, :].astype(BF)
            v = jnp.where(low, dot(coef, wt[2 * l], 1, 0), dot(coef, wt[2 * l + 1], 1, 0))
            im = v[:, CH:]
            bf[rows, :] = v[:, :CH] + sign * jnp.where(real, pltpu.roll(im, 6, 0), pltpu.roll(im, 2, 0))
        return 0
    lax.fori_loop(lax.div(pair, GROUP), DEG // 2 // GROUP, mix, 0)

    for m in range(2):
        for r in range(2):
            bfull[m, :, r * CH:(r + 1) * CH] = bf[pl.ds(2 * r + m, DEG, stride=4), :].astype(BF)

    for m in range(2):
        g = dot(ti[m], bfull[m], 1, 0)
        for r in range(2):
            for t in range(TT):
                gat[t, pl.ds(2 * m + r, DEV, stride=4), :] = g[t * DEV:(t + 1) * DEV, r * CH:(r + 1) * CH]

    for t in range(TT):
        sbuf2[:, :, t * CH:(t + 1) * CH] = gat[t].astype(BF).reshape(DEV, 4, CH)
    second = exchange(sbuf2, rbuf2, a2sem)
    loads[4].wait()
    second.wait_recv()

    rbt[...] = rbuf2[...].reshape(2 * DEG, TT * CH).T

    ysend[...] = dot(rbt[...], dfti[:, oth], 1, 0).astype(BF).reshape(TT, CH, JH)
    ycopy = [pltpu.make_async_remote_copy(ysend.at[t], y_ref.at[h * TT + t], yesem.at[t], yesem.at[TT + t],
                                          device_id=mate, device_id_type=MESH) for t in range(TT)]
    for c in ycopy:
        c.start()
    first.wait_send()
    y_ref[pl.ds(h * TT, TT)] = dot(rbt[...], dfti[:, own], 1, 0).astype(BF).reshape(TT, CH, JH)
    for c in ycopy:
        c.wait_recv()

    for c in xcopy + ycopy:
        c.wait_send()
    second.wait_send()


def solution(mesh):
    grid_spec = P('member', None, 'lat', 'lon')
    fwd_np, inv_np = dft_tables()

    def local_layer(field_in, fwd_table, inv_table, mix_weights):
        x = jnp.transpose(field_in[0], (1, 0, 2))
        mix = jnp.transpose(mix_weights, (0, 1, 3, 2)).reshape(DEG, 2 * CH, CH)
        hbm = pl.BlockSpec(memory_space=pltpu.HBM)
        dma2, dma6 = pltpu.SemaphoreType.DMA((2,)), pltpu.SemaphoreType.DMA((2 * TT,))
        y = pl.pallas_call(
            kernel,
            out_shape=jax.ShapeDtypeStruct((2 * TT, CH, JH), BF),
            in_specs=[hbm] * 6,
            out_specs=pl.BlockSpec(memory_space=pltpu.VMEM),
            scratch_shapes=[
                pltpu.VMEM((2 * TT, CH, JH), F32),
                pltpu.VMEM((2, TT * CH, JH), BF),
                pltpu.VMEM((TT * CH, JH), BF),
                pltpu.VMEM((2 * DEG, 2 * JH), BF),
                pltpu.VMEM((2 * DEG, 2 * JH), BF),
                pltpu.VMEM((2 * DEG, TT * CH), F32),
                pltpu.VMEM((DEV, 4, TT * CH), BF),
                pltpu.VMEM((DEV, 4, TT * CH), BF),
                pltpu.VMEM((2, DEG, LAT), F32),
                pltpu.VMEM((2, DEG, LAT), F32),
                pltpu.VMEM((2, DEG, LAT), BF),
                pltpu.VMEM((2, LAT, DEG), BF),
                pltpu.VMEM((WSLOTS, WCH, 2 * CH, CH), F32),
                pltpu.VMEM((DEG, CH, 2 * CH), BF),
                pltpu.VMEM((TT, 4 * DEV, CH), F32),
                pltpu.VMEM((2, LAT, 2 * CH), BF),
                pltpu.VMEM((4 * DEG, CH), F32),
                pltpu.VMEM((4 * DEG, CH), F32),
                pltpu.VMEM((2, DEG, 2 * CH), BF),
                pltpu.VMEM((DEV, 4, TT * CH), BF),
                pltpu.VMEM((DEV, 4, TT * CH), BF),
                pltpu.VMEM((TT * CH, 2 * DEG), BF),
                pltpu.VMEM((TT, CH, JH), BF),
                pltpu.SemaphoreType.DMA((5,)),
                pltpu.SemaphoreType.DMA((WSLOTS,)),
                dma6, dma2, dma2, dma6,
            ],
            compiler_params=pltpu.CompilerParams(collective_id=0, has_side_effects=True, vmem_limit_bytes=48 * 1024 * 1024),
            name="spectral_layer",
        )(*[pltpu.with_memory_space_constraint(v, pltpu.HBM) for v in (x, fwd_table, inv_table, mix, jnp.asarray(fwd_np), jnp.asarray(inv_np))])
        wave = jnp.transpose(y, (1, 0, 2))[None]
        return field_in + jax.nn.gelu(wave.astype(F32), approximate=True)

    return jax.shard_map(local_layer, mesh=mesh, in_specs=(grid_spec, P(), P(), P()), out_specs=grid_spec, check_vma=False)
```

```python
import functools
import math
import jax
import jax.numpy as jnp
import numpy as np
from jax import lax
from jax.experimental import pallas as pl
from jax.experimental.pallas import tpu as pltpu
from jax.sharding import PartitionSpec as P

MESH = pl.DeviceIdType.MESH
BF = jnp.bfloat16
F32 = jnp.float32
CH = 128
DEV = 128
CHIPS = 64
TT = 3
JH = 384
DEG = 256
LAT = 384
WCH = 8
WSLOTS = 16
EARLY = 3
BLOCKS = DEG // WCH
GROUP = 64


def chip_order():
    hops = lambda o: sum(min(v, 4 - v) for v in o)
    offsets = [(a, b, c) for a in range(4) for b in range(4) for c in range(4) if a or b or c]
    return sorted(offsets, key=lambda o: (-hops(o), o[2], o[0], o[1]))


ORDER = chip_order()
COLOURED = sorted(ORDER + [(0, 0, 0)], key=lambda o: sum(o) % 2)


def pair_of_device():
    q = np.arange(CHIPS)
    colour = (q // 16 + q // 4 % 4 + q % 4) % 2
    chip_pair = colour * (CHIPS // 2) + q // 2
    return (2 * chip_pair[:, None] + np.arange(2)[None, :]).reshape(DEV)


def dft_tables():
    lon_points, waves = 2 * JH, DEG
    phase = np.float32(2.0 * math.pi / lon_points) * (
        (np.arange(waves)[:, None] * np.arange(lon_points)[None, :]) % lon_points).astype(np.float32)
    cos_val, sin_val = np.cos(phase), np.sin(phase)
    k = np.where(np.arange(waves) == 0, 1.0, 2.0).astype(np.float32)[:, None]
    fwd = np.stack([cos_val, -sin_val], axis=1).reshape(2 * waves, lon_points)
    inv = np.stack([k * cos_val, -k * sin_val], axis=1).reshape(2 * waves, lon_points)
    rows = (4 * pair_of_device()[:, None] + np.arange(4)[None, :]).reshape(2 * waves)
    return fwd[rows].astype(BF), inv[rows].astype(BF)


def dot(a, b, ca, cb):
    return lax.dot_general(a, b, (((ca,), (cb,)), ((), ())), preferred_element_type=F32)


def kernel(x_hbm, fwd_hbm, inv_hbm, mix_hbm, dftf_hbm, dfti_hbm, out_ref,
           xv, xb, xr, dftf, dfti, acc, sbuf, rbuf, tabf, tabi, tf, ti, wbuf, wt, gat, xm,
           zf, bf, bfull, sbuf2, rbuf2, rbt, ysend, yrecv, lsem, wsem, xsem, a1sem, a2sem, yesem):
    h = lax.axis_index("lon")
    p = lax.axis_index("lat")
    d = p * 2 + h
    mate = (0, 1 - h, p)

    def wrap(v):
        return jnp.where(v >= 4, v - 4, v)
    z, y, x = lax.div(p, 16), lax.rem(lax.div(p, 4), 4), lax.rem(p, 4)
    step = lambda i: jnp.where(h == 0, i, (4 - i) % 4)
    zq = [wrap(z + step(i)) * 16 for i in range(4)]
    yq = [wrap(y + step(i)) * 4 for i in range(4)]
    xq = [wrap(x + i) for i in range(4)]

    colour = lax.rem(z + y + x, 2)
    xc = [lax.rem(x + step(i) + colour, 4) for i in range(4)]
    pair = 2 * (colour * (CHIPS // 2) + lax.div(p, 2)) + h

    loads = [
        pltpu.make_async_copy(x_hbm, xv, lsem.at[0]),
        pltpu.make_async_copy(dftf_hbm, dftf, lsem.at[1]),
        pltpu.make_async_copy(fwd_hbm.at[pl.ds(2 * pair, 2)], tabf, lsem.at[2]),
        pltpu.make_async_copy(inv_hbm.at[pl.ds(2 * pair, 2)], tabi, lsem.at[3]),
        pltpu.make_async_copy(dfti_hbm, dfti, lsem.at[4]),
    ]
    loads[0].start()

    barrier = pltpu.get_barrier_semaphore()
    for a, b, c in ORDER:
        for e in range(2):
            pl.semaphore_signal(barrier, inc=1, device_id=(0, e, zq[a] + yq[b] + xq[c]), device_id_type=MESH)
    pl.semaphore_signal(barrier, inc=1, device_id=mate, device_id_type=MESH)
    for c in loads[1:]:
        c.start()

    def wcopy(i, slot):
        return pltpu.make_async_copy(mix_hbm.at[pl.ds(i * WCH, WCH)], wbuf.at[slot], wsem.at[slot])

    loads[0].wait()
    for u in range(2):
        for t in range(TT):
            xb[u, pl.ds(t * CH, CH), :] = xv[u * TT + t].astype(BF)
    loads[1].wait()
    for i in range(WSLOTS):
        wcopy(i, i).start()
    own = pl.ds(pl.multiple_of(h * JH, JH), JH)
    oth = pl.ds(pl.multiple_of((1 - h) * JH, JH), JH)
    acc[...] = dot(dftf[:, own], xb[h], 1, 1)

    krow = lax.broadcasted_iota(jnp.int32, (LAT, LAT), 0)
    tcol = lax.broadcasted_iota(jnp.int32, (LAT, LAT), 1)
    perm = jnp.where(tcol == TT * (krow % DEV) + krow // DEV, 1.0, 0.0).astype(BF)
    loads[2].wait()
    loads[3].wait()
    for m in range(2):
        tf[m] = dot(tabf[m].astype(BF), perm, 1, 1).astype(BF)
        ti[m] = dot(perm, tabi[m].astype(BF), 1, 1).astype(BF)

    def prepare(i, refill):
        slot = lax.rem(i, WSLOTS)
        wcopy(i, slot).wait()

        def prep(l, _):
            for q in range(2):
                w = wbuf[slot, l, pl.ds(q, CH, stride=2), :]
                wt[i * WCH + l, :, q * CH:(q + 1) * CH] = w.astype(BF).T
            return 0
        lax.fori_loop(0, WCH, prep, 0, unroll=True)
        if refill:
            wcopy(i + WSLOTS, slot).start()

    def prepare_blocks(lo, hi, refill):
        def one(i, _):
            prepare(i, refill)
            return 0
        lax.fori_loop(lo, hi, one, 0)

    prepare_blocks(0, EARLY, True)
    bf[...] = jnp.zeros_like(bf)
    pl.semaphore_wait(barrier, DEV - 1)
    xcopy = [pltpu.make_async_remote_copy(xb.at[1 - h, pl.ds(t * CH, CH)], xr.at[pl.ds(t * CH, CH)], xsem.at[t], xsem.at[TT + t],
                                          device_id=mate, device_id_type=MESH) for t in range(TT)]
    for c in xcopy:
        c.start()
    for t in range(TT):
        xcopy[t].wait_recv()
    sbuf[...] = (acc[...] + dot(dftf[:, oth], xr[...], 1, 1)).astype(BF).reshape(DEV, 4, TT * CH)

    def exchange(src, dst, sem):
        for a, b, c in COLOURED:
            q = zq[a] + yq[b] + xc[c]

            def both():
                for e in range(2):
                    pltpu.make_async_remote_copy(src.at[2 * q + e], dst.at[d], sem.at[0], sem.at[1],
                                                 device_id=(0, e, q), device_id_type=MESH).start()
            if a or b:
                both()
            else:
                pl.when(q != p)(both)
        pltpu.make_async_remote_copy(src.at[d + 1 - 2 * h], dst.at[d], sem.at[0], sem.at[1],
                                     device_id=mate, device_id_type=MESH).start()
        dst[d] = src[d]
        return pltpu.make_async_remote_copy(src.at[pl.ds(0, DEV - 1)], dst.at[pl.ds(0, DEV - 1)], sem.at[0], sem.at[1],
                                            device_id=mate, device_id_type=MESH)

    first = exchange(sbuf, rbuf, a1sem)

    prepare_blocks(EARLY, BLOCKS - WSLOTS, True)
    prepare_blocks(BLOCKS - WSLOTS, BLOCKS, False)

    first.wait_recv()

    for t in range(TT):
        gat[t] = rbuf[:, :, t * CH:(t + 1) * CH].astype(F32).reshape(4 * DEV, CH)
    for m in range(2):
        for r in range(2):
            for t in range(TT):
                xm[m, t * DEV:(t + 1) * DEV, r * CH:(r + 1) * CH] = gat[t, pl.ds(2 * m + r, DEV, stride=4), :].astype(BF)
    for m in range(2):
        coef = dot(tf[m], xm[m], 1, 0)
        for r in range(2):
            zf[pl.ds(2 * r + m, DEG, stride=4), :] = coef[:, r * CH:(r + 1) * CH]

    row = lax.broadcasted_iota(jnp.int32, (8, CH), 0)
    real = lax.rem(row, 4) < 2
    sign = jnp.where(real, -1.0, 1.0)
    low = lax.broadcasted_iota(jnp.int32, (8, 2 * CH), 0) < 4

    def mix(group, _):
        for u in range(GROUP):
            l = group * GROUP + u
            rows = pl.ds(pl.multiple_of(8 * l, 8), 8)
            coef = zf[rows, :].astype(BF)
            v = jnp.where(low, dot(coef, wt[2 * l], 1, 0), dot(coef, wt[2 * l + 1], 1, 0))
            im = v[:, CH:]
            bf[rows, :] = v[:, :CH] + sign * jnp.where(real, pltpu.roll(im, 6, 0), pltpu.roll(im, 2, 0))
        return 0
    lax.fori_loop(lax.div(pair, GROUP), DEG // 2 // GROUP, mix, 0)

    for m in range(2):
        for r in range(2):
            bfull[m, :, r * CH:(r + 1) * CH] = bf[pl.ds(2 * r + m, DEG, stride=4), :].astype(BF)

    for m in range(2):
        g = dot(ti[m], bfull[m], 1, 0)
        for r in range(2):
            for t in range(TT):
                gat[t, pl.ds(2 * m + r, DEV, stride=4), :] = g[t * DEV:(t + 1) * DEV, r * CH:(r + 1) * CH]

    for t in range(TT):
        sbuf2[:, :, t * CH:(t + 1) * CH] = gat[t].astype(BF).reshape(DEV, 4, CH)
    second = exchange(sbuf2, rbuf2, a2sem)
    loads[4].wait()
    second.wait_recv()

    rbt[...] = rbuf2[...].reshape(2 * DEG, TT * CH).T

    ysend[...] = dot(rbt[...], dfti[:, oth], 1, 0).astype(BF).reshape(TT, CH, JH)
    ycopy = [pltpu.make_async_remote_copy(ysend.at[t], yrecv.at[t], yesem.at[t], yesem.at[TT + t],
                                          device_id=mate, device_id_type=MESH) for t in range(TT)]
    for c in ycopy:
        c.start()
    first.wait_send()

    def finish(base, wave):
        rows = pl.ds(base, TT)
        out_ref[rows] = xv[rows] + jax.nn.gelu(wave.astype(F32), approximate=True)

    finish(h * TT, dot(rbt[...], dfti[:, own], 1, 0).astype(BF).reshape(TT, CH, JH))
    for c in ycopy:
        c.wait_recv()
    finish((1 - h) * TT, yrecv[...])

    for c in xcopy + ycopy:
        c.wait_send()
    second.wait_send()


def solution(mesh):
    grid_spec = P('member', None, 'lat', 'lon')
    fwd_np, inv_np = dft_tables()

    def local_layer(field_in, fwd_table, inv_table, mix_weights):
        x = jnp.transpose(field_in[0], (1, 0, 2))
        mix = jnp.transpose(mix_weights, (0, 1, 3, 2)).reshape(DEG, 2 * CH, CH)
        hbm = pl.BlockSpec(memory_space=pltpu.HBM)
        dma2, dma6 = pltpu.SemaphoreType.DMA((2,)), pltpu.SemaphoreType.DMA((2 * TT,))
        out = pl.pallas_call(
            kernel,
            out_shape=jax.ShapeDtypeStruct((2 * TT, CH, JH), F32),
            in_specs=[hbm] * 6,
            out_specs=pl.BlockSpec(memory_space=pltpu.VMEM),
            scratch_shapes=[
                pltpu.VMEM((2 * TT, CH, JH), F32),
                pltpu.VMEM((2, TT * CH, JH), BF),
                pltpu.VMEM((TT * CH, JH), BF),
                pltpu.VMEM((2 * DEG, 2 * JH), BF),
                pltpu.VMEM((2 * DEG, 2 * JH), BF),
                pltpu.VMEM((2 * DEG, TT * CH), F32),
                pltpu.VMEM((DEV, 4, TT * CH), BF),
                pltpu.VMEM((DEV, 4, TT * CH), BF),
                pltpu.VMEM((2, DEG, LAT), F32),
                pltpu.VMEM((2, DEG, LAT), F32),
                pltpu.VMEM((2, DEG, LAT), BF),
                pltpu.VMEM((2, LAT, DEG), BF),
                pltpu.VMEM((WSLOTS, WCH, 2 * CH, CH), F32),
                pltpu.VMEM((DEG, CH, 2 * CH), BF),
                pltpu.VMEM((TT, 4 * DEV, CH), F32),
                pltpu.VMEM((2, LAT, 2 * CH), BF),
                pltpu.VMEM((4 * DEG, CH), F32),
                pltpu.VMEM((4 * DEG, CH), F32),
                pltpu.VMEM((2, DEG, 2 * CH), BF),
                pltpu.VMEM((DEV, 4, TT * CH), BF),
                pltpu.VMEM((DEV, 4, TT * CH), BF),
                pltpu.VMEM((TT * CH, 2 * DEG), BF),
                pltpu.VMEM((TT, CH, JH), BF),
                pltpu.VMEM((TT, CH, JH), BF),
                pltpu.SemaphoreType.DMA((5,)),
                pltpu.SemaphoreType.DMA((WSLOTS,)),
                dma6, dma2, dma2, dma6,
            ],
            compiler_params=pltpu.CompilerParams(collective_id=0, has_side_effects=True, vmem_limit_bytes=48 * 1024 * 1024),
            name="spectral_layer",
        )(*[pltpu.with_memory_space_constraint(v, pltpu.HBM) for v in (x, fwd_table, inv_table, mix, jnp.asarray(fwd_np), jnp.asarray(inv_np))])
        return jnp.transpose(out, (1, 0, 2))[None]

    return jax.shard_map(local_layer, mesh=mesh, in_specs=(grid_spec, P(), P(), P()), out_specs=grid_spec, check_vma=False)
```

```python
import functools
import math
import jax
import jax.numpy as jnp
import numpy as np
from jax import lax
from jax.experimental import pallas as pl
from jax.experimental.pallas import tpu as pltpu
from jax.sharding import PartitionSpec as P

MESH = pl.DeviceIdType.MESH
BF = jnp.bfloat16
F32 = jnp.float32
CH = 128
DEV = 128
CHIPS = 64
TT = 3
JH = 384
DEG = 256
LAT = 384
WCH = 8
WSLOTS = 16
EARLY = 5
BLOCKS = DEG // WCH
GROUP = 64


def chip_order():
    hops = lambda o: sum(min(v, 4 - v) for v in o)
    offsets = [(a, b, c) for a in range(4) for b in range(4) for c in range(4) if a or b or c]
    return sorted(offsets, key=lambda o: (-hops(o), o[2], o[0], o[1]))


ORDER = chip_order()
COLOURED = sorted(ORDER + [(0, 0, 0)], key=lambda o: sum(o) % 2)


def pair_of_device():
    q = np.arange(CHIPS)
    colour = (q // 16 + q // 4 % 4 + q % 4) % 2
    chip_pair = colour * (CHIPS // 2) + q // 2
    return (2 * chip_pair[:, None] + np.arange(2)[None, :]).reshape(DEV)


def dft_tables():
    lon_points, waves = 2 * JH, DEG
    phase = np.float32(2.0 * math.pi / lon_points) * (
        (np.arange(waves)[:, None] * np.arange(lon_points)[None, :]) % lon_points).astype(np.float32)
    cos_val, sin_val = np.cos(phase), np.sin(phase)
    k = np.where(np.arange(waves) == 0, 1.0, 2.0).astype(np.float32)[:, None]
    fwd = np.stack([cos_val, -sin_val], axis=1).reshape(2 * waves, lon_points)
    inv = np.stack([k * cos_val, -k * sin_val], axis=1).reshape(2 * waves, lon_points)
    rows = (4 * pair_of_device()[:, None] + np.arange(4)[None, :]).reshape(2 * waves)
    return fwd[rows].astype(BF), inv[rows].astype(BF)


def dot(a, b, ca, cb):
    return lax.dot_general(a, b, (((ca,), (cb,)), ((), ())), preferred_element_type=F32)


def kernel(x_hbm, fwd_hbm, inv_hbm, mix_hbm, dftf_hbm, dfti_hbm, out_ref,
           xv, xb, xr, dftf, dfti, acc, sbuf, rbuf, tabf, tabi, tf, ti, wbuf, wt, gat, xm,
           zf, bf, bfull, sbuf2, rbuf2, rbt, ysend, yrecv, lsem, wsem, xsem, a1sem, a2sem, yesem):
    h = lax.axis_index("lon")
    p = lax.axis_index("lat")
    d = p * 2 + h
    mate = (0, 1 - h, p)

    def wrap(v):
        return jnp.where(v >= 4, v - 4, v)
    z, y, x = lax.div(p, 16), lax.rem(lax.div(p, 4), 4), lax.rem(p, 4)
    step = lambda i: jnp.where(h == 0, i, (4 - i) % 4)
    zq = [wrap(z + step(i)) * 16 for i in range(4)]
    yq = [wrap(y + step(i)) * 4 for i in range(4)]
    xq = [wrap(x + i) for i in range(4)]

    colour = lax.rem(z + y + x, 2)
    xc = [lax.rem(x + step(i) + colour, 4) for i in range(4)]
    xplain = [wrap(x + step(i)) for i in range(4)]
    pair = 2 * (colour * (CHIPS // 2) + lax.div(p, 2)) + h

    loads = [
        pltpu.make_async_copy(x_hbm, xv, lsem.at[0]),
        pltpu.make_async_copy(dftf_hbm, dftf, lsem.at[1]),
        pltpu.make_async_copy(fwd_hbm.at[pl.ds(2 * pair, 2)], tabf, lsem.at[2]),
        pltpu.make_async_copy(inv_hbm.at[pl.ds(2 * pair, 2)], tabi, lsem.at[3]),
        pltpu.make_async_copy(dfti_hbm, dfti, lsem.at[4]),
    ]
    loads[0].start()

    barrier = pltpu.get_barrier_semaphore()
    for a, b, c in ORDER:
        for e in range(2):
            pl.semaphore_signal(barrier, inc=1, device_id=(0, e, zq[a] + yq[b] + xq[c]), device_id_type=MESH)
    pl.semaphore_signal(barrier, inc=1, device_id=mate, device_id_type=MESH)
    for c in loads[1:]:
        c.start()

    def wcopy(i, slot):
        return pltpu.make_async_copy(mix_hbm.at[pl.ds(i * WCH, WCH)], wbuf.at[slot], wsem.at[slot])

    loads[0].wait()
    for u in range(2):
        for t in range(TT):
            xb[u, pl.ds(t * CH, CH), :] = xv[u * TT + t].astype(BF)
    loads[1].wait()
    for i in range(WSLOTS):
        wcopy(i, i).start()
    own = pl.ds(pl.multiple_of(h * JH, JH), JH)
    oth = pl.ds(pl.multiple_of((1 - h) * JH, JH), JH)
    acc[...] = dot(dftf[:, own], xb[h], 1, 1)

    krow = lax.broadcasted_iota(jnp.int32, (LAT, LAT), 0)
    tcol = lax.broadcasted_iota(jnp.int32, (LAT, LAT), 1)
    perm = jnp.where(tcol == TT * (krow % DEV) + krow // DEV, 1.0, 0.0).astype(BF)
    loads[2].wait()
    loads[3].wait()
    for m in range(2):
        tf[m] = dot(tabf[m].astype(BF), perm, 1, 1).astype(BF)
        ti[m] = dot(perm, tabi[m].astype(BF), 1, 1).astype(BF)

    def prepare(i, refill):
        slot = lax.rem(i, WSLOTS)
        wcopy(i, slot).wait()

        def prep(l, _):
            for q in range(2):
                w = wbuf[slot, l, pl.ds(q, CH, stride=2), :]
                wt[i * WCH + l, :, q * CH:(q + 1) * CH] = w.astype(BF).T
            return 0
        lax.fori_loop(0, WCH, prep, 0, unroll=True)
        if refill:
            wcopy(i + WSLOTS, slot).start()

    def prepare_blocks(lo, hi, refill):
        def one(i, _):
            prepare(i, refill)
            return 0
        lax.fori_loop(lo, hi, one, 0)

    prepare_blocks(0, EARLY, True)
    bf[...] = jnp.zeros_like(bf)
    pl.semaphore_wait(barrier, DEV - 1)
    xcopy = [pltpu.make_async_remote_copy(xb.at[1 - h, pl.ds(t * CH, CH)], xr.at[pl.ds(t * CH, CH)], xsem.at[t], xsem.at[TT + t],
                                          device_id=mate, device_id_type=MESH) for t in range(TT)]
    for c in xcopy:
        c.start()
    for t in range(TT):
        xcopy[t].wait_recv()
    sbuf[...] = (acc[...] + dot(dftf[:, oth], xr[...], 1, 1)).astype(BF).reshape(DEV, 4, TT * CH)

    def exchange(src, dst, sem, order, xs):
        for a, b, c in order:
            q = zq[a] + yq[b] + xs[c]

            def both():
                for e in range(2):
                    pltpu.make_async_remote_copy(src.at[2 * q + e], dst.at[d], sem.at[0], sem.at[1],
                                                 device_id=(0, e, q), device_id_type=MESH).start()
            if a or b:
                both()
            else:
                pl.when(q != p)(both)
        pltpu.make_async_remote_copy(src.at[d + 1 - 2 * h], dst.at[d], sem.at[0], sem.at[1],
                                     device_id=mate, device_id_type=MESH).start()
        dst[d] = src[d]
        return pltpu.make_async_remote_copy(src.at[pl.ds(0, DEV - 1)], dst.at[pl.ds(0, DEV - 1)], sem.at[0], sem.at[1],
                                            device_id=mate, device_id_type=MESH)

    first = exchange(sbuf, rbuf, a1sem, COLOURED, xc)

    prepare_blocks(EARLY, BLOCKS - WSLOTS, True)
    prepare_blocks(BLOCKS - WSLOTS, BLOCKS, False)

    first.wait_recv()

    for t in range(TT):
        gat[t] = rbuf[:, :, t * CH:(t + 1) * CH].astype(F32).reshape(4 * DEV, CH)
    for m in range(2):
        for r in range(2):
            for t in range(TT):
                xm[m, t * DEV:(t + 1) * DEV, r * CH:(r + 1) * CH] = gat[t, pl.ds(2 * m + r, DEV, stride=4), :].astype(BF)
    for m in range(2):
        coef = dot(tf[m], xm[m], 1, 0)
        for r in range(2):
            zf[pl.ds(2 * r + m, DEG, stride=4), :] = coef[:, r * CH:(r + 1) * CH]

    row = lax.broadcasted_iota(jnp.int32, (8, CH), 0)
    real = lax.rem(row, 4) < 2
    sign = jnp.where(real, -1.0, 1.0)
    low = lax.broadcasted_iota(jnp.int32, (8, 2 * CH), 0) < 4

    def mix(group, _):
        for u in range(GROUP):
            l = group * GROUP + u
            rows = pl.ds(pl.multiple_of(8 * l, 8), 8)
            coef = zf[rows, :].astype(BF)
            v = jnp.where(low, dot(coef, wt[2 * l], 1, 0), dot(coef, wt[2 * l + 1], 1, 0))
            im = v[:, CH:]
            bf[rows, :] = v[:, :CH] + sign * jnp.where(real, pltpu.roll(im, 6, 0), pltpu.roll(im, 2, 0))
        return 0
    lax.fori_loop(lax.div(pair, GROUP), DEG // 2 // GROUP, mix, 0)

    for m in range(2):
        for r in range(2):
            bfull[m, :, r * CH:(r + 1) * CH] = bf[pl.ds(2 * r + m, DEG, stride=4), :].astype(BF)

    for m in range(2):
        g = dot(ti[m], bfull[m], 1, 0)
        for r in range(2):
            for t in range(TT):
                gat[t, pl.ds(2 * m + r, DEV, stride=4), :] = g[t * DEV:(t + 1) * DEV, r * CH:(r + 1) * CH]

    for t in range(TT):
        sbuf2[:, :, t * CH:(t + 1) * CH] = gat[t].astype(BF).reshape(DEV, 4, CH)
    second = exchange(sbuf2, rbuf2, a2sem, ORDER, xplain)
    loads[4].wait()
    second.wait_recv()

    rbt[...] = rbuf2[...].reshape(2 * DEG, TT * CH).T

    ysend[...] = dot(rbt[...], dfti[:, oth], 1, 0).astype(BF).reshape(TT, CH, JH)
    ycopy = [pltpu.make_async_remote_copy(ysend.at[t], yrecv.at[t], yesem.at[t], yesem.at[TT + t],
                                          device_id=mate, device_id_type=MESH) for t in range(TT)]
    for c in ycopy:
        c.start()
    first.wait_send()

    def finish(base, wave):
        rows = pl.ds(base, TT)
        out_ref[rows] = xv[rows] + jax.nn.gelu(wave.astype(F32), approximate=True)

    finish(h * TT, dot(rbt[...], dfti[:, own], 1, 0).astype(BF).reshape(TT, CH, JH))
    for c in ycopy:
        c.wait_recv()
    finish((1 - h) * TT, yrecv[...])

    for c in xcopy + ycopy:
        c.wait_send()
    second.wait_send()


def solution(mesh):
    grid_spec = P('member', None, 'lat', 'lon')
    fwd_np, inv_np = dft_tables()

    def local_layer(field_in, fwd_table, inv_table, mix_weights):
        x = jnp.transpose(field_in[0], (1, 0, 2))
        mix = jnp.transpose(mix_weights, (0, 1, 3, 2)).reshape(DEG, 2 * CH, CH)
        hbm = pl.BlockSpec(memory_space=pltpu.HBM)
        dma2, dma6 = pltpu.SemaphoreType.DMA((2,)), pltpu.SemaphoreType.DMA((2 * TT,))
        out = pl.pallas_call(
            kernel,
            out_shape=jax.ShapeDtypeStruct((2 * TT, CH, JH), F32),
            in_specs=[hbm] * 6,
            out_specs=pl.BlockSpec(memory_space=pltpu.VMEM),
            scratch_shapes=[
                pltpu.VMEM((2 * TT, CH, JH), F32),
                pltpu.VMEM((2, TT * CH, JH), BF),
                pltpu.VMEM((TT * CH, JH), BF),
                pltpu.VMEM((2 * DEG, 2 * JH), BF),
                pltpu.VMEM((2 * DEG, 2 * JH), BF),
                pltpu.VMEM((2 * DEG, TT * CH), F32),
                pltpu.VMEM((DEV, 4, TT * CH), BF),
                pltpu.VMEM((DEV, 4, TT * CH), BF),
                pltpu.VMEM((2, DEG, LAT), F32),
                pltpu.VMEM((2, DEG, LAT), F32),
                pltpu.VMEM((2, DEG, LAT), BF),
                pltpu.VMEM((2, LAT, DEG), BF),
                pltpu.VMEM((WSLOTS, WCH, 2 * CH, CH), F32),
                pltpu.VMEM((DEG, CH, 2 * CH), BF),
                pltpu.VMEM((TT, 4 * DEV, CH), F32),
                pltpu.VMEM((2, LAT, 2 * CH), BF),
                pltpu.VMEM((4 * DEG, CH), F32),
                pltpu.VMEM((4 * DEG, CH), F32),
                pltpu.VMEM((2, DEG, 2 * CH), BF),
                pltpu.VMEM((DEV, 4, TT * CH), BF),
                pltpu.VMEM((DEV, 4, TT * CH), BF),
                pltpu.VMEM((TT * CH, 2 * DEG), BF),
                pltpu.VMEM((TT, CH, JH), BF),
                pltpu.VMEM((TT, CH, JH), BF),
                pltpu.SemaphoreType.DMA((5,)),
                pltpu.SemaphoreType.DMA((WSLOTS,)),
                dma6, dma2, dma2, dma6,
            ],
            compiler_params=pltpu.CompilerParams(collective_id=0, has_side_effects=True, vmem_limit_bytes=48 * 1024 * 1024),
            name="spectral_layer",
        )(*[pltpu.with_memory_space_constraint(v, pltpu.HBM) for v in (x, fwd_table, inv_table, mix, jnp.asarray(fwd_np), jnp.asarray(inv_np))])
        return jnp.transpose(out, (1, 0, 2))[None]

    return jax.shard_map(local_layer, mesh=mesh, in_specs=(grid_spec, P(), P(), P()), out_specs=grid_spec, check_vma=False)
```
